32 devices in a mesh: lat: 2 (over core), lon: 4 (over y, x), lev: 4 (over z).
Axes of the slice: x: 2, y: 2, z: 4, core: 2. Of those that a mesh axis runs over, the one named last changes fastest.
Arguments:
- field_values: float32 [16, 512, 64, 128], P('lat', 'lon', 'lev'), may hold values from 0.2 to 1.8
- crowding: float32 [16, 512, 64, 128], P('lat', 'lon', 'lev'), may hold values from 0.5 to 2
Outputs:
- potential: float32 [16, 512, 64, 128], P('lat', 'lon', 'lev')
- field_values_end: float32 [16, 512, 64, 128], P('lat', 'lon', 'lev')
The draws below stay inside these ranges and needn't reach their ends.
All inputs are finite; a program needn't handle non-finite values.
Results may differ from the reference program's by a relative error of at most 0.00002.
Values sent between devices are 32-bit elements; how exact they have to be, the bound alone decides.
A program may use at most 256 MiB of HBM per device.

```python
import jax
import jax.numpy as jnp
from jax import lax

GRID_Y = 16
GRID_X = 512
GRID_Z = 64
LEVELS = 128
STEPS = 4


def block_levels(rng, shape, split, low, top_value):
    def one(axis_at, parts):
        heights = jax.random.uniform(jax.random.fold_in(jax.random.fold_in(rng, 6), axis_at), (parts,), jnp.float32, low / len(split), top_value / len(split))
        return jnp.repeat(jnp.exp(heights), shape[axis_at] // parts).reshape((-1,) + (1,) * (len(shape) - axis_at - 1))

    gain = one(*split[0])
    for cut in split[1:]:
        gain = gain * one(*cut)
    return gain


def setup_inputs(seed: int = 0) -> dict:
    splits = jax.random.split(jax.random.key(seed), 3)
    field_values = jnp.clip(0.2 + 1.5999999 * jax.random.uniform(splits[0], (GRID_Y, GRID_X, GRID_Z, LEVELS), jnp.float32) ** block_levels(splits[0], (GRID_Y, GRID_X, GRID_Z, LEVELS), ((0, 2), (1, 4), (2, 4)), -0.2, 0.2), 0.2, 1.8)
    crowding = jnp.clip(0.5 + 1.5 * jax.random.uniform(splits[1], (GRID_Y, GRID_X, GRID_Z, LEVELS), jnp.float32) ** block_levels(splits[1], (GRID_Y, GRID_X, GRID_Z, LEVELS), ((0, 2), (1, 4), (2, 4)), -0.2, 0.2), 0.5, 2.0)
    return {"field_values": field_values, "crowding": crowding}


def without_rim(values, dims):
    for dim in dims:
        values = lax.slice_in_dim(values, 1, values.shape[dim] - 1, axis=dim)
    return values


def shifted_cells(values, dim, start, dims):
    others = [other for other in dims if other != dim]
    values = without_rim(values, others)
    return lax.slice_in_dim(values, start, start + values.shape[dim] - 2, axis=dim)


def march_step(padded, crowding):
    middle = without_rim(padded, (0, 1, 2))
    lower = [shifted_cells(padded, dim, 0, (0, 1, 2)) for dim in (0, 1, 2)]
    upper = [shifted_cells(padded, dim, 2, (0, 1, 2)) for dim in (0, 1, 2)]
    spread = lower[0] + upper[0] + lower[1] + upper[1] + lower[2] + upper[2] - 6.0 * middle
    return middle + 0.1 * spread + 0.2 * middle * (1.0 - middle * crowding)


def reference(field_values, crowding):
    for step in range(STEPS):
        field_values = march_step(jnp.pad(field_values, ((1, 1), (1, 1), (1, 1), (0, 0)), mode="wrap"), crowding)
    potential = jnp.cumsum(field_values, axis=2) / GRID_Z
    return potential, field_values
```

```python
import functools

import jax
import jax.numpy as jnp
from jax import lax
from jax.experimental import pallas as pl
from jax.experimental.pallas import tpu as pltpu
from jax.sharding import PartitionSpec as P

STEPS = 4
BLOCK = 8


def row_order(rows):
    order = []
    for k in range((rows + 1) // 2):
        order.append(k)
        if rows - 1 - k != k:
            order.append(rows - 1 - k)
    return order


def kernel(
    sizes, f_hbm, c_hbm, pot_hbm, end_hbm,
    field, crowd, lat_lo, lat_hi, lon_lo, lon_hi, lev_lo, lev_hi, face_lo, face_hi, below, sums,
    in_sem, out_sem, lat_send, lat_recv, lon_send, lon_recv, lev_send, lev_recv, sum_send, sum_recv,
):
    Y, X, Z, L = crowd.shape
    order = row_order(Y)
    levels_at = lax.axis_index("lev")
    last = sizes["lev"] - 1
    scale = 1.0 / (Z * sizes["lev"])

    def beside(axis, shift):
        n = sizes[axis]
        return {axis: lax.rem(lax.axis_index(axis) + (shift + n), n)}

    def send(src, dst, send_sem, recv_sem, axis, shift):
        return pltpu.make_async_remote_copy(
            src_ref=src, dst_ref=dst, send_sem=send_sem, recv_sem=recv_sem,
            device_id=beside(axis, shift), device_id_type=pl.DeviceIdType.MESH,
        )

    f_in = [pltpu.make_async_copy(f_hbm.at[y], field.at[0, y, pl.ds(0, X)], in_sem.at[0, y]) for y in range(Y)]
    c_in = [pltpu.make_async_copy(c_hbm.at[y], crowd.at[y], in_sem.at[1, y]) for y in range(Y)]
    for y in order:
        f_in[y].start()
    for y in order:
        c_in[y].start()

    barrier = pltpu.get_barrier_semaphore()
    for axis in ("lat", "lon", "lev"):
        for shift in (-1, 1):
            pl.semaphore_signal(barrier, inc=1, device_id=beside(axis, shift), device_id_type=pl.DeviceIdType.MESH)
    pl.semaphore_wait(barrier, 6)

    def lev_copies(t, y):
        return [
            send(face_lo.at[t, y], lev_hi.at[t, y], lev_send.at[0, t, y], lev_recv.at[0, t, y], "lev", -1),
            send(face_hi.at[t, y], lev_lo.at[t, y], lev_send.at[1, t, y], lev_recv.at[1, t, y], "lev", 1),
        ]

    def lon_copies(t, y):
        row = field.at[t % 2, y]
        return [
            send(row.at[0], lon_hi.at[t, y], lon_send.at[0, t, y], lon_recv.at[0, t, y], "lon", -1),
            send(row.at[X - 1], lon_lo.at[t, y], lon_send.at[1, t, y], lon_recv.at[1, t, y], "lon", 1),
        ]

    def lat_low(t):
        return send(field.at[t % 2, 0, pl.ds(0, X)], lat_hi.at[t], lat_send.at[0, t], lat_recv.at[0, t], "lat", -1)

    def lat_high(t):
        return send(field.at[t % 2, Y - 1, pl.ds(0, X)], lat_lo.at[t], lat_send.at[1, t], lat_recv.at[1, t], "lat", 1)

    def send_row(t, y):
        for copy in lev_copies(t, y) + lon_copies(t, y):
            copy.start()
        if y == 0:
            lat_low(t).start()
        if y == Y - 1:
            lat_high(t).start()

    def sum_copy(y):
        return send(sums.at[y], below.at[y], sum_send.at[y], sum_recv.at[y], "lev", 1)

    for y in order:
        f_in[y].wait()

        @pl.loop(0, X // BLOCK)
        def _(at):
            base = pl.multiple_of(at * BLOCK, BLOCK)
            for i in range(BLOCK):
                face_lo[0, y, pl.ds(base + i, 1), :] = field[0, y, base + i, 0:1, :]
                face_hi[0, y, pl.ds(base + i, 1), :] = field[0, y, base + i, Z - 1 : Z, :]

        send_row(0, y)

    place = lax.broadcasted_iota(jnp.int32, (Z, L), 0)

    for t in range(STEPS):
        now, later = t % 2, (t + 1) % 2
        if t >= 1:
            for y in order:
                for copy in lon_copies(t - 1, y):
                    copy.wait_send()
            lat_low(t - 1).wait_send()
            lat_high(t - 1).wait_send()
        for y in order:
            if t == 0:
                c_in[y].wait()
            if y == 0:
                lat_high(t).wait_recv()
            if y == Y - 1:
                lat_low(t).wait_recv()
            for copy in lon_copies(t, y) + lev_copies(t, y):
                copy.wait_recv()
            before = field.at[now, y - 1] if y > 0 else lat_lo.at[t]
            after = field.at[now, y + 1] if y < Y - 1 else lat_hi.at[t]
            field[now, y, X] = lon_hi[t, y]

            def block(at, carry):
                left, middle = carry
                base = pl.multiple_of(at * BLOCK, BLOCK)
                for i in range(BLOCK):
                    x = base + i
                    right = field[now, y, x + 1]
                    lower = jnp.where(place == 0, lev_lo[t, y, pl.ds(x, 1), :], pltpu.roll(middle, 1, 0))
                    upper = jnp.where(place == Z - 1, lev_hi[t, y, pl.ds(x, 1), :], pltpu.roll(middle, Z - 1, 0))
                    around = (left + right) + (before[x] + after[x]) + (lower + upper)
                    new = 0.1 * around + middle * (0.6 - 0.2 * (middle * crowd[y, x]))
                    field[later, y, x] = new
                    if t < STEPS - 1:
                        face_lo[t + 1, y, pl.ds(x, 1), :] = new[0:1]
                        face_hi[t + 1, y, pl.ds(x, 1), :] = new[Z - 1 : Z]
                    else:
                        shift = 1
                        while shift < Z:
                            new = new + jnp.where(place >= shift, pltpu.roll(new, shift, 0), 0.0)
                            shift *= 2
                        crowd[y, x] = new
                        sums[y, pl.ds(x, 1), :] = new[Z - 1 : Z]
                    left, middle = middle, right
                return left, middle

            lax.fori_loop(0, X // BLOCK, block, (lon_lo[t, y], field[now, y, 0]))
            if t < STEPS - 1:
                send_row(t + 1, y)
            else:
                pltpu.make_async_copy(field.at[later, y, pl.ds(0, X)], end_hbm.at[y], out_sem.at[0, y]).start()

                @pl.when(levels_at == 0)
                def _():
                    sum_copy(y).start()

    @pl.when(levels_at == 0)
    def _():
        below[...] = jnp.zeros_like(below)

    for y in order:
        @pl.when(levels_at > 0)
        def _():
            sum_copy(y).wait_recv()

            @pl.when(levels_at < last)
            def _():
                sums[y] = sums[y] + below[y]
                sum_copy(y).start()

        @pl.loop(0, X // BLOCK)
        def _(at):
            base = pl.multiple_of(at * BLOCK, BLOCK)
            for i in range(BLOCK):
                x = base + i
                crowd[y, x] = (crowd[y, x] + below[y, pl.ds(x, 1), :]) * scale

        pltpu.make_async_copy(crowd.at[y], pot_hbm.at[y], out_sem.at[1, y]).start()

    for y in order:
        @pl.when(levels_at < last)
        def _():
            sum_copy(y).wait_send()

        pltpu.make_async_copy(field.at[STEPS % 2, y, pl.ds(0, X)], end_hbm.at[y], out_sem.at[0, y]).wait()
        pltpu.make_async_copy(crowd.at[y], pot_hbm.at[y], out_sem.at[1, y]).wait()
        for t in range(STEPS):
            for copy in lev_copies(t, y):
                copy.wait_send()
        for copy in lon_copies(STEPS - 1, y):
            copy.wait_send()
    lat_low(STEPS - 1).wait_send()
    lat_high(STEPS - 1).wait_send()


def per_device(sizes, field_values, crowding):
    Y, X, Z, L = field_values.shape
    f32 = jnp.float32
    dma = pltpu.SemaphoreType.DMA
    anywhere = pl.BlockSpec(memory_space=pl.ANY)
    shape = jax.ShapeDtypeStruct(field_values.shape, f32)
    return pl.pallas_call(
        functools.partial(kernel, sizes),
        out_shape=(shape, shape),
        in_specs=[anywhere, anywhere],
        out_specs=(anywhere, anywhere),
        scratch_shapes=[
            pltpu.VMEM((2, Y, X + 1, Z, L), f32),
            pltpu.VMEM((Y, X, Z, L), f32),
            pltpu.VMEM((STEPS, X, Z, L), f32),
            pltpu.VMEM((STEPS, X, Z, L), f32),
            pltpu.VMEM((STEPS, Y, Z, L), f32),
            pltpu.VMEM((STEPS, Y, Z, L), f32),
            pltpu.VMEM((STEPS, Y, X, L), f32),
            pltpu.VMEM((STEPS, Y, X, L), f32),
            pltpu.VMEM((STEPS, Y, X, L), f32),
            pltpu.VMEM((STEPS, Y, X, L), f32),
            pltpu.VMEM((Y, X, L), f32),
            pltpu.VMEM((Y, X, L), f32),
            dma((2, Y)),
            dma((2, Y)),
            dma((2, STEPS)),
            dma((2, STEPS)),
            dma((2, STEPS, Y)),
            dma((2, STEPS, Y)),
            dma((2, STEPS, Y)),
            dma((2, STEPS, Y)),
            dma((Y,)),
            dma((Y,)),
        ],
        compiler_params=pltpu.CompilerParams(
            collective_id=0, has_side_effects=True, vmem_limit_bytes=60 * 1024 * 1024
        ),
    )(field_values, crowding)


def solution(mesh):
    return jax.shard_map(
        functools.partial(per_device, dict(mesh.shape)),
        mesh=mesh,
        in_specs=(P("lat", "lon", "lev", None), P("lat", "lon", "lev", None)),
        out_specs=(P("lat", "lon", "lev", None), P("lat", "lon", "lev", None)),
        check_vma=False,
    )
```

```python
import functools

import jax
import jax.numpy as jnp
from jax import lax
from jax.experimental import pallas as pl
from jax.experimental.pallas import tpu as pltpu
from jax.sharding import PartitionSpec as P

STEPS = 4
BLOCK = 8


def row_order(rows):
    order = []
    for k in range((rows + 1) // 2):
        order.append(k)
        if rows - 1 - k != k:
            order.append(rows - 1 - k)
    return order


def kernel(
    sizes, f_hbm, c_hbm, end_hbm, below_hbm,
    field, crowd, lat_lo, lat_hi, lon_lo, lon_hi, lev_lo, lev_hi, face_lo, face_hi, below, sums,
    in_sem, out_sem, lat_send, lat_recv, lon_send, lon_recv, lev_send, lev_recv, sum_send, sum_recv,
):
    Y, X, Z, L = crowd.shape
    order = row_order(Y)
    levels_at = lax.axis_index("lev")
    last = sizes["lev"] - 1

    def beside(axis, shift):
        n = sizes[axis]
        return {axis: lax.rem(lax.axis_index(axis) + (shift + n), n)}

    def send(src, dst, send_sem, recv_sem, axis, shift):
        return pltpu.make_async_remote_copy(
            src_ref=src, dst_ref=dst, send_sem=send_sem, recv_sem=recv_sem,
            device_id=beside(axis, shift), device_id_type=pl.DeviceIdType.MESH,
        )

    f_in = [pltpu.make_async_copy(f_hbm.at[y], field.at[0, y, pl.ds(0, X)], in_sem.at[0, y]) for y in range(Y)]
    c_in = [pltpu.make_async_copy(c_hbm.at[y], crowd.at[y], in_sem.at[1, y]) for y in range(Y)]
    for y in order:
        f_in[y].start()
    for y in order:
        c_in[y].start()

    barrier = pltpu.get_barrier_semaphore()
    for axis in ("lat", "lon", "lev"):
        for shift in (-1, 1):
            pl.semaphore_signal(barrier, inc=1, device_id=beside(axis, shift), device_id_type=pl.DeviceIdType.MESH)
    pl.semaphore_wait(barrier, 6)

    def lev_copies(t, y):
        return [
            send(face_lo.at[t, y], lev_hi.at[t, y], lev_send.at[0, t, y], lev_recv.at[0, t, y], "lev", -1),
            send(face_hi.at[t, y], lev_lo.at[t, y], lev_send.at[1, t, y], lev_recv.at[1, t, y], "lev", 1),
        ]

    def lon_copies(t, y):
        row = field.at[t % 2, y]
        return [
            send(row.at[0], lon_hi.at[t, y], lon_send.at[0, t, y], lon_recv.at[0, t, y], "lon", -1),
            send(row.at[X - 1], lon_lo.at[t, y], lon_send.at[1, t, y], lon_recv.at[1, t, y], "lon", 1),
        ]

    def lat_low(t):
        return send(field.at[t % 2, 0, pl.ds(0, X)], lat_hi.at[t], lat_send.at[0, t], lat_recv.at[0, t], "lat", -1)

    def lat_high(t):
        return send(field.at[t % 2, Y - 1, pl.ds(0, X)], lat_lo.at[t], lat_send.at[1, t], lat_recv.at[1, t], "lat", 1)

    def send_row(t, y):
        for copy in lev_copies(t, y) + lon_copies(t, y):
            copy.start()
        if y == 0:
            lat_low(t).start()
        if y == Y - 1:
            lat_high(t).start()

    def sum_copy(y):
        return send(sums.at[y], below.at[y], sum_send.at[y], sum_recv.at[y], "lev", 1)

    for y in order:
        f_in[y].wait()

        @pl.loop(0, X // BLOCK)
        def _(at):
            base = pl.multiple_of(at * BLOCK, BLOCK)
            for i in range(BLOCK):
                face_lo[0, y, pl.ds(base + i, 1), :] = field[0, y, base + i, 0:1, :]
                face_hi[0, y, pl.ds(base + i, 1), :] = field[0, y, base + i, Z - 1 : Z, :]

        send_row(0, y)

    place = lax.broadcasted_iota(jnp.int32, (Z, L), 0)

    for t in range(STEPS):
        now, later = t % 2, (t + 1) % 2
        if t >= 1:
            for y in order:
                for copy in lon_copies(t - 1, y):
                    copy.wait_send()
            lat_low(t - 1).wait_send()
            lat_high(t - 1).wait_send()
        for y in order:
            if t == 0:
                c_in[y].wait()
            if y == 0:
                lat_high(t).wait_recv()
            if y == Y - 1:
                lat_low(t).wait_recv()
            for copy in lon_copies(t, y) + lev_copies(t, y):
                copy.wait_recv()
            before = field.at[now, y - 1] if y > 0 else lat_lo.at[t]
            after = field.at[now, y + 1] if y < Y - 1 else lat_hi.at[t]
            field[now, y, X] = lon_hi[t, y]

            def block(at, carry):
                left, middle = carry
                base = pl.multiple_of(at * BLOCK, BLOCK)
                for i in range(BLOCK):
                    x = base + i
                    right = field[now, y, x + 1]
                    lower = jnp.where(place == 0, lev_lo[t, y, pl.ds(x, 1), :], pltpu.roll(middle, 1, 0))
                    upper = jnp.where(place == Z - 1, lev_hi[t, y, pl.ds(x, 1), :], pltpu.roll(middle, Z - 1, 0))
                    around = (left + right) + (before[x] + after[x]) + (lower + upper)
                    new = 0.1 * around + middle * (0.6 - 0.2 * (middle * crowd[y, x]))
                    field[later, y, x] = new
                    if t < STEPS - 1:
                        face_lo[t + 1, y, pl.ds(x, 1), :] = new[0:1]
                        face_hi[t + 1, y, pl.ds(x, 1), :] = new[Z - 1 : Z]
                    else:
                        sums[y, pl.ds(x, 1), :] = jnp.sum(new, axis=0, keepdims=True)
                    left, middle = middle, right
                return left, middle

            lax.fori_loop(0, X // BLOCK, block, (lon_lo[t, y], field[now, y, 0]))
            if t < STEPS - 1:
                send_row(t + 1, y)
            else:
                pltpu.make_async_copy(field.at[later, y, pl.ds(0, X)], end_hbm.at[y], out_sem.at[0, y]).start()

                @pl.when(levels_at == 0)
                def _():
                    sum_copy(y).start()

    @pl.when(levels_at == 0)
    def _():
        below[...] = jnp.zeros_like(below)

    for y in order:
        @pl.when(levels_at > 0)
        def _():
            sum_copy(y).wait_recv()

            @pl.when(levels_at < last)
            def _():
                sums[y] = sums[y] + below[y]
                sum_copy(y).start()

        pltpu.make_async_copy(below.at[y], below_hbm.at[y], out_sem.at[1, y]).start()

    for y in order:
        @pl.when(levels_at < last)
        def _():
            sum_copy(y).wait_send()

        pltpu.make_async_copy(field.at[STEPS % 2, y, pl.ds(0, X)], end_hbm.at[y], out_sem.at[0, y]).wait()
        pltpu.make_async_copy(below.at[y], below_hbm.at[y], out_sem.at[1, y]).wait()
        for t in range(STEPS):
            for copy in lev_copies(t, y):
                copy.wait_send()
        for copy in lon_copies(STEPS - 1, y):
            copy.wait_send()
    lat_low(STEPS - 1).wait_send()
    lat_high(STEPS - 1).wait_send()


def finish(scale, end_ref, below_ref, pot_ref, copy_ref):
    _, X, Z, L = end_ref.shape
    place = lax.broadcasted_iota(jnp.int32, (Z, L), 0)

    @pl.loop(0, X // BLOCK)
    def _(at):
        base = pl.multiple_of(at * BLOCK, BLOCK)
        for i in range(BLOCK):
            x = base + i
            here = end_ref[0, x]
            copy_ref[0, x] = here
            shift = 1
            while shift < Z:
                here = here + jnp.where(place >= shift, pltpu.roll(here, shift, 0), 0.0)
                shift *= 2
            pot_ref[0, x] = (here + below_ref[0, pl.ds(x, 1), :]) * scale


def per_device(sizes, field_values, crowding):
    Y, X, Z, L = field_values.shape
    f32 = jnp.float32
    dma = pltpu.SemaphoreType.DMA
    anywhere = pl.BlockSpec(memory_space=pl.ANY)
    shape = jax.ShapeDtypeStruct(field_values.shape, f32)
    end, below = pl.pallas_call(
        functools.partial(kernel, sizes),
        out_shape=(shape, jax.ShapeDtypeStruct((Y, X, L), f32)),
        in_specs=[anywhere, anywhere],
        out_specs=(anywhere, anywhere),
        scratch_shapes=[
            pltpu.VMEM((2, Y, X + 1, Z, L), f32),
            pltpu.VMEM((Y, X, Z, L), f32),
            pltpu.VMEM((STEPS, X, Z, L), f32),
            pltpu.VMEM((STEPS, X, Z, L), f32),
            pltpu.VMEM((STEPS, Y, Z, L), f32),
            pltpu.VMEM((STEPS, Y, Z, L), f32),
            pltpu.VMEM((STEPS, Y, X, L), f32),
            pltpu.VMEM((STEPS, Y, X, L), f32),
            pltpu.VMEM((STEPS, Y, X, L), f32),
            pltpu.VMEM((STEPS, Y, X, L), f32),
            pltpu.VMEM((Y, X, L), f32),
            pltpu.VMEM((Y, X, L), f32),
            dma((2, Y)),
            dma((2, Y)),
            dma((2, STEPS)),
            dma((2, STEPS)),
            dma((2, STEPS, Y)),
            dma((2, STEPS, Y)),
            dma((2, STEPS, Y)),
            dma((2, STEPS, Y)),
            dma((Y,)),
            dma((Y,)),
        ],
        compiler_params=pltpu.CompilerParams(
            collective_id=0, has_side_effects=True, vmem_limit_bytes=60 * 1024 * 1024
        ),
    )(field_values, crowding)
    width = X // 2
    cells = pl.BlockSpec((1, width, Z, L), lambda y, x: (y, x, 0, 0))
    return pl.pallas_call(
        functools.partial(finish, 1.0 / (Z * sizes["lev"])),
        grid=(Y, X // width),
        out_shape=(shape, shape),
        in_specs=[cells, pl.BlockSpec((1, width, L), lambda y, x: (y, x, 0))],
        out_specs=(cells, cells),
    )(end, below)


def solution(mesh):
    return jax.shard_map(
        functools.partial(per_device, dict(mesh.shape)),
        mesh=mesh,
        in_specs=(P("lat", "lon", "lev", None), P("lat", "lon", "lev", None)),
        out_specs=(P("lat", "lon", "lev", None), P("lat", "lon", "lev", None)),
        check_vma=False,
    )
```
